32 devices in a mesh: scan: 2 (over x), slab: 16 (over z, y, core).
Axes of the slice: x: 2, y: 2, z: 4, core: 2. Of those that a mesh axis runs over, the one named last changes fastest.
Arguments:
- kernels: bfloat16 [4, 6, 6, 6, 16384], P('scan', None, None, None, 'slab'), parts along dimension 0, may hold values from -0.013671875 to 0.013671875
Outputs:
- gram: float32 [4, 32, 1, 192, 1024], P('scan', 'slab'), parts along dimension 0
The draws below stay inside these ranges and needn't reach their ends.
There are 2 independent parts, one for each index of `scan`. The reference program is written for one: setup_inputs(seed, part) draws one part's arguments, and reference() takes and returns one part's arrays. A program takes and returns all parts, laid end to end along the dimension named above; each array names one. Nothing has to cross between parts.
All inputs are finite; a program needn't handle non-finite values.
Results may differ from the reference program's by a relative error of at most 0.0023.
Values may be sent and summed in bfloat16 or wider, within the bound.
A program may use at most 128 MiB of HBM per device.

```python
import math
import jax
import jax.numpy as jnp
from jax import lax

COILS = 32
NKER = 512
TAP = 6
NY = 256
NZ = 192
YW = 1
NX = 32
YLO = 127


def levels(key, dims, cuts, least, high):
    gain, own = 1.0, jax.random.fold_in(key, 6)
    for dim, blocks in cuts:
        draws = jnp.exp(jax.random.uniform(jax.random.fold_in(own, dim), (blocks,), jnp.float32, least / len(cuts), high / len(cuts)))
        gain = gain * jnp.repeat(draws, dims[dim] // blocks).reshape([-1 if axis == dim else 1 for axis in range(len(dims))])
    return gain


def centred(stream_key, extent, width, most, cuts=(), kind=jnp.bfloat16):
    values = width * jax.random.normal(stream_key, extent, jnp.float32)
    if cuts:
        values = values * levels(stream_key, extent, cuts, -0.22, 0.18)
    return jnp.clip(values, -most, most).astype(kind)


def setup_inputs(seed: int = 0, part: int = 0) -> dict:
    splits = jax.random.split(jax.random.key(seed), 2)
    part_keys = jax.random.split(jax.random.fold_in(splits[1], part), 2)
    kernels = centred(part_keys[0], (2, TAP, TAP, TAP, NKER * COILS), (2 * TAP * TAP * TAP * NKER) ** -0.5, 0.013671875, ((4, 16),))
    return {"kernels": kernels}


full_turn = 2.0 * math.pi


def first_segment(columns, planes, length):
    shape = (planes.shape[0],) + columns.shape[2:]
    real_sum = jnp.zeros(shape, jnp.float32)
    imag_sum = jnp.zeros(shape, jnp.float32)
    for offset in range(columns.shape[1]):
        angle = ((planes * offset) % length).astype(jnp.float32) * (full_turn / length)
        cosine = jnp.cos(angle)[:, None, None, None]
        sine = jnp.sin(angle)[:, None, None, None]
        real_tap = columns[0, offset].astype(jnp.float32)[None]
        imag_tap = columns[1, offset].astype(jnp.float32)[None]
        real_sum = real_sum + real_tap * cosine - imag_tap * sine
        imag_sum = imag_sum + real_tap * sine + imag_tap * cosine
    return jnp.stack([real_sum, imag_sum]).astype(jnp.bfloat16)


def second_segment(first, rows, length):
    shape = (first.shape[1], rows.shape[0], first.shape[3], first.shape[4])
    real_sum = jnp.zeros(shape, jnp.float32)
    imag_sum = jnp.zeros(shape, jnp.float32)
    for offset in range(first.shape[2]):
        angle = ((rows * offset) % length).astype(jnp.float32) * (full_turn / length)
        cosine = jnp.cos(angle)[None, :, None, None]
        sine = jnp.sin(angle)[None, :, None, None]
        real_tap = first[0, :, offset].astype(jnp.float32)[:, None]
        imag_tap = first[1, :, offset].astype(jnp.float32)[:, None]
        real_sum = real_sum + real_tap * cosine - imag_tap * sine
        imag_sum = imag_sum + real_tap * sine + imag_tap * cosine
    return jnp.stack([real_sum, imag_sum], axis=2).astype(jnp.bfloat16)


def depth_table(length, taps):
    depth = jnp.arange(length, dtype=jnp.int32)
    offsets = jnp.arange(taps, dtype=jnp.int32)
    angle = ((depth[:, None] * offsets[None, :]) % length).astype(jnp.float32) * (full_turn / length)
    cosine = jnp.cos(angle)
    sine = jnp.sin(angle)
    table = jnp.stack([jnp.stack([cosine, -sine], axis=1), jnp.stack([sine, cosine], axis=1)], axis=1)
    return table.reshape(length * 2, 2 * taps).astype(jnp.bfloat16)


def gram_block(images):
    wide = images.astype(jnp.float32)
    full = jnp.einsum('vrck,vsdk->vrcsd', wide, wide)
    real_part = full[:, 0, :, 0, :] + full[:, 1, :, 1, :]
    imag_part = full[:, 0, :, 1, :] - full[:, 1, :, 0, :]
    count = images.shape[0]
    return jnp.stack([real_part, imag_part]).reshape(2, count, COILS * COILS)


def reference(kernels):
    table = depth_table(NZ, TAP)
    rows = (YLO + jnp.arange(YW, dtype=jnp.int32)).astype(jnp.int32)

    def one_plane(plane):
        first = first_segment(kernels, plane[None].astype(jnp.int32), NX)
        second = second_segment(first, rows, NY)[0]
        second = second.reshape(YW, 2 * TAP, NKER * COILS)
        images = jnp.einsum('mn,bnq->bmq', table.astype(jnp.float32), second.astype(jnp.float32))
        images = images.astype(jnp.bfloat16).reshape(YW * NZ, 2, COILS, NKER)
        return gram_block(images).reshape(2, YW, NZ, COILS * COILS)

    planes = jnp.arange(NX, dtype=jnp.int32)
    result = lax.map(one_plane, planes)
    return jnp.moveaxis(result, 0, 1)
```

```python
import functools
import math

import jax
import jax.numpy as jnp
import numpy as np
from jax import lax
from jax.experimental import pallas as pl
from jax.experimental.pallas import tpu as pltpu
from jax.sharding import PartitionSpec as P

COILS = 32
TAP = 6
NY = 256
NZ = 192
XD = 2
YLO = 127
SUB = 8
ROW = 2 * TAP
PADROW = 16
LANES = 128

full_turn = 2.0 * math.pi


def split(value):
    value = np.asarray(value, np.float32)
    high = value.astype(jnp.bfloat16)
    low = (value - high.astype(np.float32)).astype(jnp.bfloat16)
    return high, low


def plane_matrix(planes, halves):
    count = planes // XD
    angle = (np.arange(planes)[:, None] * np.arange(TAP)[None] % planes) * (full_turn / planes)
    cosine, sine = np.cos(angle), np.sin(angle)
    base = np.zeros((planes, 2, TAP, 2, TAP, SUB))
    for w in range(TAP):
        base[:, 0, w, 0, :, w] = cosine
        base[:, 0, w, 1, :, w] = -sine
        base[:, 1, w, 0, :, w] = sine
        base[:, 1, w, 1, :, w] = cosine
    high, low = split(base.reshape(count, XD * ROW, 2 * TAP * SUB))
    terms = np.concatenate([high, low, high], axis=2)
    depth = terms.shape[2]
    full = np.zeros((count, halves, XD * ROW, halves, depth), terms.dtype)
    for half in range(halves):
        full[:, half, :, half, :] = terms
    return full.reshape(count * halves * XD * ROW, halves * depth)


def place_matrix(halves):
    full = np.zeros((XD, halves, PADROW, halves, XD, ROW), np.float32)
    for plane in range(XD):
        for half in range(halves):
            for row in range(ROW):
                full[plane, half, row, half, plane, row] = 1
    return full.reshape(XD * halves * PADROW, halves * XD * ROW).astype(jnp.bfloat16)


def swap_matrix():
    full = np.zeros((ROW, COILS, COILS, PADROW), np.float32)
    for row in range(ROW):
        for coil in range(COILS):
            full[row, coil, coil, row] = 1
    return full.reshape(ROW * COILS, COILS * PADROW).astype(jnp.bfloat16)


def depth_matrix():
    angle = (np.arange(NZ)[:, None] * np.arange(TAP)[None] % NZ).astype(np.float32) * np.float32(full_turn / NZ)
    cosine = np.cos(angle).astype(jnp.bfloat16).astype(np.float32)
    sine = np.sin(angle).astype(jnp.bfloat16).astype(np.float32)
    alpha = np.concatenate([cosine, -sine], axis=1)
    beta = np.concatenate([sine, cosine], axis=1)
    full = np.zeros((2, NZ, ROW, PADROW), np.float32)
    full[0, :, :, :ROW] = alpha[:, :, None] * alpha[:, None, :] + beta[:, :, None] * beta[:, None, :]
    full[1, :, :, :ROW] = beta[:, :, None] * alpha[:, None, :] - alpha[:, :, None] * beta[:, None, :]
    high, low = split(full.reshape(2 * NZ, ROW * PADROW))
    return np.concatenate([high, low, high], axis=1)


def exchange_kernel(count, halves, width, kernels, planes, place, out, taps, terms, sent, held, send_sem, recv_sem):
    me = lax.axis_index("slab")
    barrier = pltpu.get_barrier_semaphore()

    def greet(step, carry):
        pl.semaphore_signal(
            barrier, inc=1, device_id={"slab": lax.rem(me + step, count)}, device_id_type=pl.DeviceIdType.MESH
        )
        return carry

    lax.fori_loop(1, count, greet, 0)

    lanes = kernels.shape[4]
    taps[...] = jnp.zeros_like(taps)
    for u in range(TAP):
        real_sum = jnp.zeros((TAP, lanes), jnp.float32)
        imag_sum = jnp.zeros((TAP, lanes), jnp.float32)
        for v in range(TAP):
            angle = (v * YLO % NY) * (full_turn / NY)
            cosine, sine = math.cos(angle), math.sin(angle)
            real_tap = kernels[0, u, v].astype(jnp.float32)
            imag_tap = kernels[1, u, v].astype(jnp.float32)
            real_sum = real_sum + real_tap * cosine - imag_tap * sine
            imag_sum = imag_sum + real_tap * sine + imag_tap * cosine
        taps[u * SUB : u * SUB + TAP, :] = real_sum
        taps[(TAP + u) * SUB : (TAP + u) * SUB + TAP, :] = imag_sum
    depth = 2 * TAP * SUB
    for half in range(halves):
        value = taps[:, half * width : (half + 1) * width]
        high = value.astype(jnp.bfloat16)
        low = (value - high.astype(jnp.float32)).astype(jnp.bfloat16)
        start = half * 3 * depth
        terms[start : start + depth, :] = high
        terms[start + depth : start + 2 * depth, :] = high
        terms[start + 2 * depth : start + 3 * depth, :] = low
    rows = halves * XD * ROW
    images = jnp.dot(planes[...], terms[...], preferred_element_type=jnp.float32)
    sent[...] = images.astype(jnp.bfloat16).reshape(count, rows, width)

    pl.semaphore_wait(barrier, count - 1)

    def copy_to(step):
        return pltpu.make_async_remote_copy(
            src_ref=sent.at[lax.rem(me + step, count)],
            dst_ref=held.at[step],
            send_sem=send_sem.at[step],
            recv_sem=recv_sem.at[step],
            device_id={"slab": lax.rem(me + step, count)},
            device_id_type=pl.DeviceIdType.MESH,
        )

    def send(step, carry):
        copy_to(step).start()
        return carry

    lax.fori_loop(1, count, send, 0)

    column_count = count * lanes // COILS

    def settle(source, block):
        moved = jnp.dot(place[...], block, preferred_element_type=jnp.float32).astype(jnp.bfloat16)
        size = halves * PADROW
        coil = source * lanes // column_count
        column = pl.multiple_of(lax.rem(source * lanes, column_count), width)
        for plane in range(XD):
            out[plane, pl.ds(pl.multiple_of(coil * PADROW, PADROW), size), pl.ds(column, width)] = moved[
                plane * size : (plane + 1) * size
            ]

    settle(me, sent[me])

    def receive(step, carry):
        copy_to(step).wait_recv()
        settle(lax.rem(me - step + count, count), held[step])
        return carry

    lax.fori_loop(1, count, receive, 0)

    def drain(step, carry):
        copy_to(step).wait_send()
        return carry

    lax.fori_loop(1, count, drain, 0)


def gram_kernel(taps, swap, table, out, spread, right):
    group = LANES // COILS
    ordered = jnp.dot(swap[...], taps[0], preferred_element_type=jnp.float32).astype(jnp.bfloat16)
    for row in range(ROW):
        block = ordered[row * COILS : (row + 1) * COILS]
        for copy in range(group):
            start = (row * group + copy) * COILS
            spread[start : start + COILS, :] = block
    lane = lax.broadcasted_iota(jnp.int32, (PADROW, LANES), 1) // COILS
    size = ROW * PADROW
    pair = 2
    for row in range(0, ROW, pair):
        products = lax.dot_general(
            taps[0],
            spread[row * LANES : (row + pair) * LANES, :],
            (((1,), (1,)), ((), ())),
            preferred_element_type=jnp.float32,
        )
        for side in range(pair):
            start = (row + side) * PADROW
            for block in range(COILS // group):
                picked = None
                for member in range(group):
                    first = (block * group + member) * PADROW
                    piece = products[first : first + PADROW, side * LANES : (side + 1) * LANES]
                    picked = piece if picked is None else jnp.where(lane == member, piece, picked)
                high = picked.astype(jnp.bfloat16)
                low = (picked - high.astype(jnp.float32)).astype(jnp.bfloat16)
                columns = slice(block * LANES, (block + 1) * LANES)
                right[start : start + PADROW, columns] = high
                right[size + start : size + start + PADROW, columns] = high
                right[2 * size + start : 2 * size + start + PADROW, columns] = low
    for part in range(2):
        out[part, 0, 0] = jnp.dot(
            table[part * NZ : (part + 1) * NZ, :], right[...], preferred_element_type=jnp.float32
        )


def local(kernels):
    count = lax.axis_size("slab")
    lanes = kernels.shape[4]
    column_count = count * lanes // COILS
    halves = max(1, lanes // column_count)
    width = lanes // halves
    rows = halves * XD * ROW
    depth = 2 * TAP * SUB
    vmem = pl.BlockSpec(memory_space=pltpu.VMEM)
    taps = pl.pallas_call(
        functools.partial(exchange_kernel, count, halves, width),
        out_shape=jax.ShapeDtypeStruct((XD, COILS * PADROW, column_count), jnp.bfloat16),
        in_specs=[vmem] * 3,
        out_specs=vmem,
        scratch_shapes=[
            pltpu.VMEM((depth, lanes), jnp.float32),
            pltpu.VMEM((halves * 3 * depth, width), jnp.bfloat16),
            pltpu.VMEM((count, rows, width), jnp.bfloat16),
            pltpu.VMEM((count, rows, width), jnp.bfloat16),
            pltpu.SemaphoreType.DMA((count,)),
            pltpu.SemaphoreType.DMA((count,)),
        ],
        compiler_params=pltpu.CompilerParams(collective_id=0, has_side_effects=True),
        name="exchange",
    )(kernels, jnp.asarray(plane_matrix(XD * count, halves)), jnp.asarray(place_matrix(halves)))
    wide = COILS * PADROW
    return pl.pallas_call(
        gram_kernel,
        grid=(XD,),
        out_shape=jax.ShapeDtypeStruct((2, XD, 1, NZ, COILS * COILS), jnp.float32),
        in_specs=[
            pl.BlockSpec((1, wide, column_count), lambda plane: (plane, 0, 0)),
            pl.BlockSpec((ROW * COILS, wide), lambda plane: (0, 0)),
            pl.BlockSpec((2 * NZ, 3 * ROW * PADROW), lambda plane: (0, 0)),
        ],
        out_specs=pl.BlockSpec((2, 1, 1, NZ, COILS * COILS), lambda plane: (0, plane, 0, 0, 0)),
        scratch_shapes=[
            pltpu.VMEM((ROW * LANES, column_count), jnp.bfloat16),
            pltpu.VMEM((3 * ROW * PADROW, COILS * COILS), jnp.bfloat16),
        ],
        name="gram",
    )(taps, jnp.asarray(swap_matrix()), jnp.asarray(depth_matrix()))


def solution(mesh):
    return jax.shard_map(
        local,
        mesh=mesh,
        in_specs=(P("scan", None, None, None, "slab"),),
        out_specs=P("scan", "slab", None, None, None),
        check_vma=False,
    )
```

```python
import functools
import math

import jax
import jax.numpy as jnp
import numpy as np
from jax import lax
from jax.experimental import pallas as pl
from jax.experimental.pallas import tpu as pltpu
from jax.sharding import PartitionSpec as P

COILS = 32
TAP = 6
NY = 256
NZ = 192
XD = 2
YLO = 127
SUB = 8
ROW = 2 * TAP
PADROW = 16
LANES = 128

full_turn = 2.0 * math.pi


def split(value):
    value = np.asarray(value, np.float32)
    high = value.astype(jnp.bfloat16)
    low = (value - high.astype(np.float32)).astype(jnp.bfloat16)
    return high, low


def plane_matrix(planes):
    count = planes // XD
    grid = np.arange(planes)
    taps = np.arange(TAP)
    first = (grid[:, None] * taps[None] % planes) * (full_turn / planes)
    second = (taps * YLO % NY) * (full_turn / NY)
    angle = first[:, :, None] + second[None, None, :]
    cosine, sine = np.cos(angle), np.sin(angle)
    base = np.zeros((planes, 2, TAP, TAP, TAP, TAP, 2))
    for w in range(TAP):
        base[:, 0, w, :, :, w, 0] = cosine
        base[:, 0, w, :, :, w, 1] = -sine
        base[:, 1, w, :, :, w, 0] = sine
        base[:, 1, w, :, :, w, 1] = cosine
    base = base.reshape(count, XD, ROW, 2 * TAP**3)
    tiles = [base[:, 0, :SUB], base[:, 0, SUB:], base[:, 1, SUB:], base[:, 1, :SUB]]
    high, low = split(np.concatenate(tiles, axis=1).reshape(count * XD * ROW, 2 * TAP**3))
    return np.concatenate([high, low], axis=1)


def message_rows(plane, parts):
    if parts == 1:
        return [(0, row) for row in range(SUB)] + [
            (0, SUB + row % 4) if (row >= 4) == (plane == 1) else None for row in range(SUB)
        ]
    whole = [(part, row) for part in range(parts) for row in range(SUB)]
    return whole + [(part, row) for part in range(parts) for row in range(SUB, ROW)]


def place_matrix(parts):
    size = len(message_rows(0, parts))
    full = np.zeros((XD, parts * PADROW, size), np.float32)
    for plane in range(XD):
        for index, entry in enumerate(message_rows(plane, parts)):
            if entry is not None:
                full[plane, entry[0] * PADROW + entry[1], index] = 1
    return full.astype(jnp.bfloat16)


def pack(block, parts, width):
    first, mixed, second = block[:SUB], block[SUB : 2 * SUB], block[2 * SUB :]
    if parts == 1:
        return [jnp.concatenate([first, mixed]), jnp.concatenate([second, mixed])]
    cut = lambda value, part: value[:, part * width : (part + 1) * width]
    lower = lax.broadcasted_iota(jnp.int32, (SUB, width), 0) < SUB // 2
    turned = pltpu.roll(mixed, SUB // 2, axis=0)
    packed = []
    for plane, whole in enumerate((first, second)):
        rows = [cut(whole, part) for part in range(parts)]
        under, over = (mixed, turned) if plane == 0 else (turned, mixed)
        for part in range(0, parts, 2):
            rows.append(jnp.where(lower, cut(under, part), cut(over, part + 1)))
        packed.append(jnp.concatenate(rows))
    return packed


def swap_matrix():
    full = np.zeros((ROW, COILS, COILS, PADROW), np.float32)
    for row in range(ROW):
        for coil in range(COILS):
            full[row, coil, coil, row] = 1
    return full.reshape(ROW * COILS, COILS * PADROW).astype(jnp.bfloat16)


def depth_matrix():
    angle = (np.arange(NZ)[:, None] * np.arange(TAP)[None] % NZ).astype(np.float32) * np.float32(full_turn / NZ)
    cosine = np.cos(angle).astype(jnp.bfloat16).astype(np.float32)
    sine = np.sin(angle).astype(jnp.bfloat16).astype(np.float32)
    alpha = np.concatenate([cosine, -sine], axis=1)
    beta = np.concatenate([sine, cosine], axis=1)
    full = np.zeros((2, NZ, ROW, PADROW), np.float32)
    full[0, :, :, :ROW] = alpha[:, :, None] * alpha[:, None, :] + beta[:, :, None] * beta[:, None, :]
    full[1, :, :, :ROW] = beta[:, :, None] * alpha[:, None, :] - alpha[:, :, None] * beta[:, None, :]
    high, low = split(full.reshape(2 * NZ, ROW * PADROW))
    return np.stack([high, low]).reshape(2, 2, NZ, ROW * PADROW)


def exchange_kernel(
    count, parts, width, kernels, planes, place, swap, right, sent, held, taps, spread, send_sem, recv_sem
):
    me = lax.axis_index("slab")
    barrier = pltpu.get_barrier_semaphore()

    def greet(step, carry):
        pl.semaphore_signal(
            barrier, inc=1, device_id={"slab": lax.rem(me + step, count)}, device_id_type=pl.DeviceIdType.MESH
        )
        return carry

    lax.fori_loop(1, count, greet, 0)

    lanes = kernels.shape[2]
    depth = 2 * TAP**3
    rows = XD * ROW
    columns = kernels[...].reshape(depth, lanes)
    images = jnp.dot(planes[:, :depth], columns, preferred_element_type=jnp.float32)
    images = images + jnp.dot(planes[:, depth:], columns, preferred_element_type=jnp.float32)
    for target in range(count):
        for plane, message in enumerate(pack(images[target * rows : (target + 1) * rows], parts, width)):
            sent[plane, target] = message.astype(jnp.bfloat16)

    pl.semaphore_wait(barrier, count - 1)

    def copy_to(plane, step):
        target = lax.rem(me + step, count)
        return pltpu.make_async_remote_copy(
            src_ref=sent.at[plane, target],
            dst_ref=held.at[plane, step],
            send_sem=send_sem.at[plane, step],
            recv_sem=recv_sem.at[plane, step],
            device_id={"slab": target},
            device_id_type=pl.DeviceIdType.MESH,
        )

    for plane in range(XD):

        def send(step, carry):
            copy_to(plane, step).start()
            return carry

        lax.fori_loop(1, count, send, 0)

    column_count = count * lanes // COILS

    def settle(plane, source, block):
        moved = jnp.dot(place[plane], block, preferred_element_type=jnp.float32).astype(jnp.bfloat16)
        for part in range(parts):
            start = source * lanes + part * width
            coil = start // column_count
            column = pl.multiple_of(lax.rem(start, column_count), width)
            taps[pl.ds(pl.multiple_of(coil * PADROW, PADROW), PADROW), pl.ds(column, width)] = moved[
                part * PADROW : (part + 1) * PADROW
            ]

    for plane in range(XD):
        settle(plane, me, sent[plane, me])

        def receive(step, carry):
            copy_to(plane, step).wait_recv()
            settle(plane, lax.rem(me - step + count, count), held[plane, step])
            return carry

        lax.fori_loop(1, count, receive, 0)
        gram_products(taps, swap, right.at[plane], spread)

    for plane in range(XD):

        def drain(step, carry):
            copy_to(plane, step).wait_send()
            return carry

        lax.fori_loop(1, count, drain, 0)


def gram_products(taps, swap, right, spread):
    group = LANES // COILS
    ordered = jnp.dot(swap[...], taps[...], preferred_element_type=jnp.float32).astype(jnp.bfloat16)
    for row in range(ROW):
        block = ordered[row * COILS : (row + 1) * COILS]
        for copy in range(group):
            start = (row * group + copy) * COILS
            spread[start : start + COILS, :] = block
    lane = lax.broadcasted_iota(jnp.int32, (PADROW, LANES), 1) // COILS
    pair = 2
    for row in range(0, ROW, pair):
        products = lax.dot_general(
            taps[...],
            spread[row * LANES : (row + pair) * LANES, :],
            (((1,), (1,)), ((), ())),
            preferred_element_type=jnp.float32,
        )
        for side in range(pair):
            start = (row + side) * PADROW
            for block in range(COILS // group):
                picked = None
                for member in range(group):
                    first = (block * group + member) * PADROW
                    piece = products[first : first + PADROW, side * LANES : (side + 1) * LANES]
                    picked = piece if picked is None else jnp.where(lane == member, piece, picked)
                high = picked.astype(jnp.bfloat16)
                low = (picked - high.astype(jnp.float32)).astype(jnp.bfloat16)
                columns = slice(block * LANES, (block + 1) * LANES)
                right[0, start : start + PADROW, columns] = high
                right[1, start : start + PADROW, columns] = low


def depth_kernel(right, table, out):
    left = jnp.concatenate([table[0, 0], table[1, 0], table[0, 0]], axis=1)
    stack = jnp.concatenate([right[0, 0], right[0, 0], right[0, 1]], axis=0)
    out[0, 0, 0] = jnp.dot(left, stack, preferred_element_type=jnp.float32)


def local(kernels):
    count = lax.axis_size("slab")
    lanes = kernels.shape[4]
    column_count = count * lanes // COILS
    parts = 4 if lanes % (4 * LANES) == 0 else 1
    width = lanes // parts
    size = len(message_rows(0, parts))
    depth = ROW * PADROW
    vmem = pl.BlockSpec(memory_space=pltpu.VMEM)
    columns = jnp.transpose(kernels, (1, 2, 3, 0, 4)).reshape(TAP**3, 2, lanes)
    right = pl.pallas_call(
        functools.partial(exchange_kernel, count, parts, width),
        out_shape=jax.ShapeDtypeStruct((XD, 2, depth, COILS * COILS), jnp.bfloat16),
        in_specs=[vmem] * 4,
        out_specs=vmem,
        scratch_shapes=[
            pltpu.VMEM((XD, count, size, width), jnp.bfloat16),
            pltpu.VMEM((XD, count, size, width), jnp.bfloat16),
            pltpu.VMEM((COILS * PADROW, column_count), jnp.bfloat16),
            pltpu.VMEM((ROW * LANES, column_count), jnp.bfloat16),
            pltpu.SemaphoreType.DMA((XD, count)),
            pltpu.SemaphoreType.DMA((XD, count)),
        ],
        compiler_params=pltpu.CompilerParams(collective_id=0, has_side_effects=True),
        name="exchange",
    )(columns, jnp.asarray(plane_matrix(XD * count)), jnp.asarray(place_matrix(parts)), jnp.asarray(swap_matrix()))
    return pl.pallas_call(
        depth_kernel,
        grid=(XD, 2),
        out_shape=jax.ShapeDtypeStruct((2, XD, 1, NZ, COILS * COILS), jnp.float32),
        in_specs=[
            pl.BlockSpec((1, 2, depth, COILS * COILS), lambda plane, part: (plane, 0, 0, 0)),
            pl.BlockSpec((2, 1, NZ, depth), lambda plane, part: (0, part, 0, 0)),
        ],
        out_specs=pl.BlockSpec((1, 1, 1, NZ, COILS * COILS), lambda plane, part: (part, plane, 0, 0, 0)),
        name="depth",
    )(right, jnp.asarray(depth_matrix()))


def solution(mesh):
    return jax.shard_map(
        local,
        mesh=mesh,
        in_specs=(P("scan", None, None, None, "slab"),),
        out_specs=P("scan", "slab", None, None, None),
        check_vma=False,
    )
```

```python
import functools
import math

import jax
import jax.numpy as jnp
import numpy as np
from jax import lax
from jax.experimental import pallas as pl
from jax.experimental.pallas import tpu as pltpu
from jax.sharding import PartitionSpec as P

COILS = 32
TAP = 6
NY = 256
NZ = 192
XD = 2
YLO = 127
SUB = 8
ROW = 2 * TAP
PADROW = 16
LANES = 128

full_turn = 2.0 * math.pi


def split(value):
    value = np.asarray(value, np.float32)
    high = value.astype(jnp.bfloat16)
    low = (value - high.astype(np.float32)).astype(jnp.bfloat16)
    return high, low


def plane_matrix(planes):
    count = planes // XD
    grid = np.arange(planes)
    taps = np.arange(TAP)
    first = (grid[:, None] * taps[None] % planes) * (full_turn / planes)
    second = (taps * YLO % NY) * (full_turn / NY)
    angle = first[:, :, None] + second[None, None, :]
    cosine, sine = np.cos(angle), np.sin(angle)
    base = np.zeros((planes, 2, TAP, TAP, TAP, TAP, 2))
    for w in range(TAP):
        base[:, 0, w, :, :, w, 0] = cosine
        base[:, 0, w, :, :, w, 1] = -sine
        base[:, 1, w, :, :, w, 0] = sine
        base[:, 1, w, :, :, w, 1] = cosine
    base = base.reshape(count, XD, ROW, 2 * TAP**3)
    tiles = [base[:, 0, :SUB], base[:, 0, SUB:], base[:, 1, SUB:], base[:, 1, :SUB]]
    high, low = split(np.concatenate(tiles, axis=1).reshape(count * XD * ROW, 2 * TAP**3))
    return np.concatenate([high, low], axis=1)


def slot(row):
    return row // TAP * SUB + TAP - 1 - row % TAP


def message_rows(plane, parts):
    if parts == 1:
        return [(0, row) for row in range(SUB)] + [
            (0, SUB + row % 4) if (row >= 4) == (plane == 1) else None for row in range(SUB)
        ]
    whole = [(part, row) for part in range(parts) for row in range(SUB)]
    return whole + [(part, row) for part in range(parts) for row in range(SUB, ROW)]


def place_matrix(parts):
    size = len(message_rows(0, parts))
    full = np.zeros((XD, parts * PADROW, size), np.float32)
    for plane in range(XD):
        for index, entry in enumerate(message_rows(plane, parts)):
            if entry is not None:
                full[plane, entry[0] * PADROW + slot(entry[1]), index] = 1
    return full.astype(jnp.bfloat16)


def pack(block, parts, width):
    first, mixed, second = block[:SUB], block[SUB : 2 * SUB], block[2 * SUB :]
    if parts == 1:
        return [jnp.concatenate([first, mixed]), jnp.concatenate([second, mixed])]
    cut = lambda value, part: value[:, part * width : (part + 1) * width]
    lower = lax.broadcasted_iota(jnp.int32, (SUB, width), 0) < SUB // 2
    turned = pltpu.roll(mixed, SUB // 2, axis=0)
    packed = []
    for plane, whole in enumerate((first, second)):
        rows = [cut(whole, part) for part in range(parts)]
        under, over = (mixed, turned) if plane == 0 else (turned, mixed)
        for part in range(0, parts, 2):
            rows.append(jnp.where(lower, cut(under, part), cut(over, part + 1)))
        packed.append(jnp.concatenate(rows))
    return packed


def swap_matrix():
    full = np.zeros((ROW, COILS, COILS, PADROW), np.float32)
    for row in range(ROW):
        for coil in range(COILS):
            full[row, coil, coil, slot(row)] = 1
    return full.reshape(ROW * COILS, COILS * PADROW).astype(jnp.bfloat16)


def depth_matrix():
    shift = np.arange(2 * TAP - 1) - (TAP - 1)
    angle = (np.arange(NZ)[:, None] * shift[None] % NZ) * (full_turn / NZ)
    full = np.zeros((2, NZ, 2, PADROW))
    full[0, :, 0, : 2 * TAP - 1] = np.cos(angle)
    full[0, :, 1, : 2 * TAP - 1] = -np.sin(angle)
    full[1, :, 0, : 2 * TAP - 1] = np.sin(angle)
    full[1, :, 1, : 2 * TAP - 1] = np.cos(angle)
    high, low = split(full.reshape(2 * NZ, 2 * PADROW))
    return np.concatenate([high, low, high], axis=1)


def exchange_kernel(
    count, parts, width, kernels, planes, place, swap, right, sent, held, taps, send_sem, recv_sem
):
    me = lax.axis_index("slab")
    barrier = pltpu.get_barrier_semaphore()

    def greet(step, carry):
        pl.semaphore_signal(
            barrier, inc=1, device_id={"slab": lax.rem(me + step, count)}, device_id_type=pl.DeviceIdType.MESH
        )
        return carry

    lax.fori_loop(1, count, greet, 0)

    lanes = kernels.shape[2]
    depth = 2 * TAP**3
    rows = XD * ROW
    columns = kernels[...].reshape(depth, lanes)
    images = jnp.dot(planes[:, :depth], columns, preferred_element_type=jnp.float32)
    images = images + jnp.dot(planes[:, depth:], columns, preferred_element_type=jnp.float32)
    for target in range(count):
        for plane, message in enumerate(pack(images[target * rows : (target + 1) * rows], parts, width)):
            sent[plane, target] = message.astype(jnp.bfloat16)

    pl.semaphore_wait(barrier, count - 1)

    def copy_to(plane, step):
        target = lax.rem(me + step, count)
        return pltpu.make_async_remote_copy(
            src_ref=sent.at[plane, target],
            dst_ref=held.at[plane, step],
            send_sem=send_sem.at[plane, step],
            recv_sem=recv_sem.at[plane, step],
            device_id={"slab": target},
            device_id_type=pl.DeviceIdType.MESH,
        )

    for plane in range(XD):

        def send(step, carry):
            copy_to(plane, step).start()
            return carry

        lax.fori_loop(1, count, send, 0)

    column_count = count * lanes // COILS

    def settle(plane, source, block):
        moved = jnp.dot(place[plane], block, preferred_element_type=jnp.float32).astype(jnp.bfloat16)
        for part in range(parts):
            start = source * lanes + part * width
            coil = start // column_count
            column = pl.multiple_of(lax.rem(start, column_count), width)
            taps[pl.ds(pl.multiple_of(coil * PADROW, PADROW), PADROW), pl.ds(column, width)] = moved[
                part * PADROW : (part + 1) * PADROW
            ]

    for plane in range(XD):
        settle(plane, me, sent[plane, me])

        def receive(step, carry):
            copy_to(plane, step).wait_recv()
            settle(plane, lax.rem(me - step + count, count), held[plane, step])
            return carry

        lax.fori_loop(1, count, receive, 0)
        gram_products(taps, swap, right.at[plane])

    for plane in range(XD):

        def drain(step, carry):
            copy_to(plane, step).wait_send()
            return carry

        lax.fori_loop(1, count, drain, 0)


def gram_products(taps, swap, right):
    group = LANES // COILS
    ordered = jnp.dot(swap[...], taps[...], preferred_element_type=jnp.float32).astype(jnp.bfloat16)
    products = lax.dot_general(
        taps[...], ordered, (((1,), (1,)), ((), ())), preferred_element_type=jnp.float32
    )
    lane = lax.broadcasted_iota(jnp.int32, (SUB, LANES), 1) // COILS
    level = lax.broadcasted_iota(jnp.int32, (SUB, LANES), 0)
    for block in range(COILS // group):
        picked = [[None] * ROW for _ in range(2)]
        for part in range(2):
            for row in range(ROW):
                place, start = row % group, row // group * LANES
                for member in range(group):
                    first = (block * group + member) * PADROW + part * SUB
                    piece = products[first : first + SUB, start : start + LANES]
                    turn = (member - place) % group * COILS
                    piece = pltpu.roll(piece, turn, axis=1) if turn else piece
                    known = picked[part][row]
                    picked[part][row] = piece if known is None else jnp.where(lane == member, piece, known)
        columns = slice(block * LANES, (block + 1) * LANES)
        for part in range(2):
            under, over = None, jnp.zeros((SUB, LANES), jnp.float32)
            for w in range(TAP):
                if part == 0:
                    value = picked[0][w] + picked[1][TAP + w]
                else:
                    value = picked[0][TAP + w] - picked[1][w]
                if w == 0:
                    under = value
                    continue
                value = pltpu.roll(value, w, axis=0)
                under = under + jnp.where(level >= w, value, 0.0)
                over = over + jnp.where(level < w, value, 0.0)
            right[part * PADROW : part * PADROW + SUB, columns] = under
            right[part * PADROW + SUB : (part + 1) * PADROW, columns] = over


def depth_kernel(right, table, out):
    value = right[0]
    high = value.astype(jnp.bfloat16)
    low = (value - high.astype(jnp.float32)).astype(jnp.bfloat16)
    stack = jnp.concatenate([high, high, low], axis=0)
    result = jnp.dot(table[...], stack, preferred_element_type=jnp.float32)
    out[0, 0, 0] = result[:NZ]
    out[1, 0, 0] = result[NZ:]


def local(kernels):
    count = lax.axis_size("slab")
    lanes = kernels.shape[4]
    column_count = count * lanes // COILS
    parts = 4 if lanes % (4 * LANES) == 0 else 1
    width = lanes // parts
    size = len(message_rows(0, parts))
    pairs = COILS * COILS
    vmem = pl.BlockSpec(memory_space=pltpu.VMEM)
    columns = jnp.transpose(kernels, (1, 2, 3, 0, 4)).reshape(TAP**3, 2, lanes)
    right = pl.pallas_call(
        functools.partial(exchange_kernel, count, parts, width),
        out_shape=jax.ShapeDtypeStruct((XD, 2 * PADROW, pairs), jnp.float32),
        in_specs=[vmem] * 4,
        out_specs=vmem,
        scratch_shapes=[
            pltpu.VMEM((XD, count, size, width), jnp.bfloat16),
            pltpu.VMEM((XD, count, size, width), jnp.bfloat16),
            pltpu.VMEM((COILS * PADROW, column_count), jnp.bfloat16),
            pltpu.SemaphoreType.DMA((XD, count)),
            pltpu.SemaphoreType.DMA((XD, count)),
        ],
        compiler_params=pltpu.CompilerParams(collective_id=0, has_side_effects=True),
        name="exchange",
    )(columns, jnp.asarray(plane_matrix(XD * count)), jnp.asarray(place_matrix(parts)), jnp.asarray(swap_matrix()))
    return pl.pallas_call(
        depth_kernel,
        grid=(XD, 2),
        out_shape=jax.ShapeDtypeStruct((2, XD, 1, NZ, pairs), jnp.float32),
        in_specs=[
            pl.BlockSpec((1, 2 * PADROW, pairs // 2), lambda plane, side: (plane, 0, side)),
            pl.BlockSpec((2 * NZ, 6 * PADROW), lambda plane, side: (0, 0)),
        ],
        out_specs=pl.BlockSpec((2, 1, 1, NZ, pairs // 2), lambda plane, side: (0, plane, 0, 0, side)),
        name="depth",
    )(right, jnp.asarray(depth_matrix()))


def solution(mesh):
    return jax.shard_map(
        local,
        mesh=mesh,
        in_specs=(P("scan", None, None, None, "slab"),),
        out_specs=P("scan", "slab", None, None, None),
        check_vma=False,
    )
```

```python
import functools
import math

import jax
import jax.numpy as jnp
import numpy as np
from jax import lax
from jax.experimental import pallas as pl
from jax.experimental.pallas import tpu as pltpu
from jax.sharding import PartitionSpec as P

COILS = 32
TAP = 6
NY = 256
NZ = 192
XD = 2
YLO = 127
SUB = 8
ROW = 2 * TAP
PADROW = 16
LANES = 128

full_turn = 2.0 * math.pi


def split(value):
    value = np.asarray(value, np.float32)
    high = value.astype(jnp.bfloat16)
    low = (value - high.astype(np.float32)).astype(jnp.bfloat16)
    return high, low


def plane_matrix(planes):
    count = planes // XD
    grid = np.arange(planes)
    taps = np.arange(TAP)
    first = (grid[:, None] * taps[None] % planes) * (full_turn / planes)
    second = (taps * YLO % NY) * (full_turn / NY)
    angle = first[:, :, None] + second[None, None, :]
    cosine, sine = np.cos(angle), np.sin(angle)
    base = np.zeros((planes, 2, TAP, TAP, TAP, TAP, 2))
    for w in range(TAP):
        base[:, 0, w, :, :, w, 0] = cosine
        base[:, 0, w, :, :, w, 1] = -sine
        base[:, 1, w, :, :, w, 0] = sine
        base[:, 1, w, :, :, w, 1] = cosine
    base = base.reshape(count, XD, ROW, 2 * TAP**3)
    tiles = [base[:, 0, :SUB], base[:, 0, SUB:], base[:, 1, SUB:], base[:, 1, :SUB]]
    high, low = split(np.concatenate(tiles, axis=1).reshape(count * XD * ROW, 2 * TAP**3))
    return np.concatenate([high, low], axis=1)


def slot(row):
    return row // TAP * SUB + TAP - 1 - row % TAP


def message_rows(plane, parts):
    if parts == 1:
        return [(0, row) for row in range(SUB)] + [
            (0, SUB + row % 4) if (row >= 4) == (plane == 1) else None for row in range(SUB)
        ]
    whole = [(part, row) for part in range(parts) for row in range(SUB)]
    return whole + [(part, row) for part in range(parts) for row in range(SUB, ROW)]


def place_matrix(parts):
    size = len(message_rows(0, parts))
    full = np.zeros((XD, parts * PADROW, size), np.float32)
    for plane in range(XD):
        for index, entry in enumerate(message_rows(plane, parts)):
            if entry is not None:
                full[plane, entry[0] * PADROW + slot(entry[1]), index] = 1
    return full.astype(jnp.bfloat16)


def pack(block, parts, width):
    first, mixed, second = block[:SUB], block[SUB : 2 * SUB], block[2 * SUB :]
    if parts == 1:
        return [jnp.concatenate([first, mixed]), jnp.concatenate([second, mixed])]
    cut = lambda value, part: value[:, part * width : (part + 1) * width]
    lower = lax.broadcasted_iota(jnp.int32, (SUB, width), 0) < SUB // 2
    turned = pltpu.roll(mixed, SUB // 2, axis=0)
    packed = []
    for plane, whole in enumerate((first, second)):
        rows = [cut(whole, part) for part in range(parts)]
        under, over = (mixed, turned) if plane == 0 else (turned, mixed)
        for part in range(0, parts, 2):
            rows.append(jnp.where(lower, cut(under, part), cut(over, part + 1)))
        packed.append(jnp.concatenate(rows))
    return packed


def swap_matrix():
    full = np.zeros((ROW, COILS, COILS, PADROW), np.float32)
    for row in range(ROW):
        for coil in range(COILS):
            full[row, coil, coil, slot(row)] = 1
    return full.reshape(ROW * COILS, COILS * PADROW).astype(jnp.bfloat16)


def depth_matrix():
    shift = np.arange(2 * TAP - 1) - (TAP - 1)
    angle = (np.arange(NZ)[:, None] * shift[None] % NZ) * (full_turn / NZ)
    full = np.zeros((2, NZ, 2, PADROW))
    full[0, :, 0, : 2 * TAP - 1] = np.cos(angle)
    full[0, :, 1, : 2 * TAP - 1] = -np.sin(angle)
    full[1, :, 0, : 2 * TAP - 1] = np.sin(angle)
    full[1, :, 1, : 2 * TAP - 1] = np.cos(angle)
    high, low = split(full.reshape(2 * NZ, 2 * PADROW))
    return np.concatenate([high, low, high], axis=1).reshape(2, NZ, 6 * PADROW)


def exchange_kernel(
    count, parts, width, kernels, planes, place, swap, right, sent, held, taps, send_sem, recv_sem
):
    me = lax.axis_index("slab")
    barrier = pltpu.get_barrier_semaphore()

    def greet(step, carry):
        pl.semaphore_signal(
            barrier, inc=1, device_id={"slab": lax.rem(me + step, count)}, device_id_type=pl.DeviceIdType.MESH
        )
        return carry

    lax.fori_loop(1, count, greet, 0)

    def partner(step, sign):
        if count & (count - 1) == 0:
            return me ^ step
        return lax.rem(me + sign * step + count, count)

    lanes = kernels.shape[2]
    depth = 2 * TAP**3
    rows = XD * ROW
    columns = kernels[...].reshape(depth, lanes)
    images = jnp.dot(planes[:, :depth], columns, preferred_element_type=jnp.float32)
    images = images + jnp.dot(planes[:, depth:], columns, preferred_element_type=jnp.float32)
    for target in range(count):
        for plane, message in enumerate(pack(images[target * rows : (target + 1) * rows], parts, width)):
            sent[plane, target] = message.astype(jnp.bfloat16)

    pl.semaphore_wait(barrier, count - 1)

    def copy_to(plane, step):
        target = partner(step, 1)
        return pltpu.make_async_remote_copy(
            src_ref=sent.at[plane, target],
            dst_ref=held.at[plane, step],
            send_sem=send_sem.at[plane, step],
            recv_sem=recv_sem.at[plane, step],
            device_id={"slab": target},
            device_id_type=pl.DeviceIdType.MESH,
        )

    for plane in range(XD):

        def send(step, carry):
            copy_to(plane, step).start()
            return carry

        lax.fori_loop(1, count, send, 0)

    column_count = count * lanes // COILS

    def settle(plane, source, block):
        moved = jnp.dot(place[plane], block, preferred_element_type=jnp.float32).astype(jnp.bfloat16)
        for part in range(parts):
            start = source * lanes + part * width
            coil = start // column_count
            column = pl.multiple_of(lax.rem(start, column_count), width)
            taps[pl.ds(pl.multiple_of(coil * PADROW, PADROW), PADROW), pl.ds(column, width)] = moved[
                part * PADROW : (part + 1) * PADROW
            ]

    for plane in range(XD):
        settle(plane, me, sent[plane, me])

        def receive(step, carry):
            copy_to(plane, step).wait_recv()
            settle(plane, partner(step, -1), held[plane, step])
            return carry

        lax.fori_loop(1, count, receive, 0)
        gram_products(taps, swap, right.at[plane])

    for plane in range(XD):

        def drain(step, carry):
            copy_to(plane, step).wait_send()
            return carry

        lax.fori_loop(1, count, drain, 0)


def gram_products(taps, swap, right):
    group = LANES // COILS
    ordered = jnp.dot(swap[...], taps[...], preferred_element_type=jnp.float32).astype(jnp.bfloat16)
    products = lax.dot_general(
        taps[...], ordered, (((1,), (1,)), ((), ())), preferred_element_type=jnp.float32
    )
    lane = lax.broadcasted_iota(jnp.int32, (SUB, LANES), 1) // COILS
    level = lax.broadcasted_iota(jnp.int32, (SUB, LANES), 0)
    for block in range(COILS // group):
        picked = [[None] * ROW for _ in range(2)]
        for part in range(2):
            for row in range(ROW):
                place, start = row % group, row // group * LANES
                for member in range(group):
                    first = (block * group + member) * PADROW + part * SUB
                    piece = products[first : first + SUB, start : start + LANES]
                    turn = (member - place) % group * COILS
                    piece = pltpu.roll(piece, turn, axis=1) if turn else piece
                    known = picked[part][row]
                    picked[part][row] = piece if known is None else jnp.where(lane == member, piece, known)
        columns = slice(block * LANES, (block + 1) * LANES)
        for part in range(2):
            under, over = None, jnp.zeros((SUB, LANES), jnp.float32)
            for w in range(TAP):
                if part == 0:
                    value = picked[0][w] + picked[1][TAP + w]
                else:
                    value = picked[0][TAP + w] - picked[1][w]
                if w == 0:
                    under = value
                    continue
                value = pltpu.roll(value, w, axis=0)
                under = under + jnp.where(level >= w, value, 0.0)
                over = over + jnp.where(level < w, value, 0.0)
            right[part * PADROW : part * PADROW + SUB, columns] = under
            right[part * PADROW + SUB : (part + 1) * PADROW, columns] = over


def depth_kernel(right, table, out):
    value = right[0]
    high = value.astype(jnp.bfloat16)
    low = (value - high.astype(jnp.float32)).astype(jnp.bfloat16)
    stack = jnp.concatenate([high, high, low], axis=0)
    for part in range(2):
        out[part, 0, 0] = jnp.dot(table[part], stack, preferred_element_type=jnp.float32)


def local(kernels):
    count = lax.axis_size("slab")
    lanes = kernels.shape[4]
    column_count = count * lanes // COILS
    parts = 4 if lanes % (4 * LANES) == 0 else 1
    width = lanes // parts
    size = len(message_rows(0, parts))
    pairs = COILS * COILS
    vmem = pl.BlockSpec(memory_space=pltpu.VMEM)
    columns = jnp.transpose(kernels, (1, 2, 3, 0, 4)).reshape(TAP**3, 2, lanes)
    right = pl.pallas_call(
        functools.partial(exchange_kernel, count, parts, width),
        out_shape=jax.ShapeDtypeStruct((XD, 2 * PADROW, pairs), jnp.float32),
        in_specs=[vmem] * 4,
        out_specs=vmem,
        scratch_shapes=[
            pltpu.VMEM((XD, count, size, width), jnp.bfloat16),
            pltpu.VMEM((XD, count, size, width), jnp.bfloat16),
            pltpu.VMEM((COILS * PADROW, column_count), jnp.bfloat16),
            pltpu.SemaphoreType.DMA((XD, count)),
            pltpu.SemaphoreType.DMA((XD, count)),
        ],
        compiler_params=pltpu.CompilerParams(collective_id=0, has_side_effects=True),
        name="exchange",
    )(columns, jnp.asarray(plane_matrix(XD * count)), jnp.asarray(place_matrix(parts)), jnp.asarray(swap_matrix()))
    return pl.pallas_call(
        depth_kernel,
        grid=(XD, 2),
        out_shape=jax.ShapeDtypeStruct((2, XD, 1, NZ, pairs), jnp.float32),
        in_specs=[
            pl.BlockSpec((1, 2 * PADROW, pairs), lambda plane, side: (plane, 0, 0)),
            pl.BlockSpec((2, NZ // 2, 6 * PADROW), lambda plane, side: (0, side, 0)),
        ],
        out_specs=pl.BlockSpec((2, 1, 1, NZ // 2, pairs), lambda plane, side: (0, plane, 0, side, 0)),
        name="depth",
    )(right, jnp.asarray(depth_matrix()))


def solution(mesh):
    return jax.shard_map(
        local,
        mesh=mesh,
        in_specs=(P("scan", None, None, None, "slab"),),
        out_specs=P("scan", "slab", None, None, None),
        check_vma=False,
    )
```

```python
import functools
import math

import jax
import jax.numpy as jnp
import numpy as np
from jax import lax
from jax.experimental import pallas as pl
from jax.experimental.pallas import tpu as pltpu
from jax.sharding import PartitionSpec as P

COILS = 32
TAP = 6
NY = 256
NZ = 192
XD = 2
YLO = 127
SUB = 8
ROW = 2 * TAP
PADROW = 16
LANES = 128

full_turn = 2.0 * math.pi


def split(value):
    value = np.asarray(value, np.float32)
    high = value.astype(jnp.bfloat16)
    low = (value - high.astype(np.float32)).astype(jnp.bfloat16)
    return high, low


def plane_matrix(planes):
    count = planes // XD
    grid = np.arange(planes)
    taps = np.arange(TAP)
    first = (grid[:, None] * taps[None] % planes) * (full_turn / planes)
    second = (taps * YLO % NY) * (full_turn / NY)
    angle = first[:, :, None] + second[None, None, :]
    cosine, sine = np.cos(angle), np.sin(angle)
    base = np.zeros((planes, 2, TAP, TAP, TAP, TAP, 2))
    for w in range(TAP):
        base[:, 0, w, :, :, w, 0] = cosine
        base[:, 0, w, :, :, w, 1] = -sine
        base[:, 1, w, :, :, w, 0] = sine
        base[:, 1, w, :, :, w, 1] = cosine
    base = base.reshape(count, XD, ROW, 2 * TAP**3)
    base = np.concatenate([base, base[:, :, SUB:]], axis=2).swapaxes(0, 1)
    high, low = split(base.reshape(XD, count * PADROW, 2 * TAP**3))
    return np.concatenate([high, low], axis=2)


def slot(row):
    return row // TAP * SUB + TAP - 1 - row % TAP


def message_rows(parts):
    if parts == 1:
        return [(0, row) for row in range(ROW)] + [None] * (PADROW - ROW)
    whole = [(part, row) for part in range(parts) for row in range(SUB)]
    return whole + [(part, row) for part in range(parts) for row in range(SUB, ROW)]


def place_matrix(parts):
    rows = message_rows(parts)
    full = np.zeros((parts * PADROW, len(rows)), np.float32)
    for index, entry in enumerate(rows):
        if entry is not None:
            full[entry[0] * PADROW + slot(entry[1]), index] = 1
    return full.astype(jnp.bfloat16)


def pack(block, parts, width):
    if parts == 1:
        return block
    cut = lambda value, part: value[:, part * width : (part + 1) * width]
    whole, mixed = block[:SUB], block[SUB:]
    lower = lax.broadcasted_iota(jnp.int32, (SUB, width), 0) < SUB // 2
    rows = [cut(whole, part) for part in range(parts)]
    for part in range(0, parts, 2):
        rows.append(jnp.where(lower, cut(mixed, part), cut(mixed, part + 1)))
    return jnp.concatenate(rows)


def swap_matrix():
    full = np.zeros((ROW, COILS, COILS, PADROW), np.float32)
    for row in range(ROW):
        for coil in range(COILS):
            full[row, coil, coil, slot(row)] = 1
    return full.reshape(ROW * COILS, COILS * PADROW).astype(jnp.bfloat16)


def depth_matrix():
    shift = np.arange(2 * TAP - 1) - (TAP - 1)
    angle = (np.arange(NZ)[:, None] * shift[None] % NZ) * (full_turn / NZ)
    full = np.zeros((2, NZ, 2, PADROW))
    full[0, :, 0, : 2 * TAP - 1] = np.cos(angle)
    full[0, :, 1, : 2 * TAP - 1] = -np.sin(angle)
    full[1, :, 0, : 2 * TAP - 1] = np.sin(angle)
    full[1, :, 1, : 2 * TAP - 1] = np.cos(angle)
    high, low = split(full.reshape(2 * NZ, 2 * PADROW))
    return np.concatenate([high, low, high], axis=1)


def exchange_kernel(
    count, parts, width, kernels, planes, place, swap, right, sent, held, taps, send_sem, recv_sem
):
    me = lax.axis_index("slab")
    barrier = pltpu.get_barrier_semaphore()

    def greet(step, carry):
        pl.semaphore_signal(
            barrier, inc=1, device_id={"slab": lax.rem(me + step, count)}, device_id_type=pl.DeviceIdType.MESH
        )
        return carry

    lax.fori_loop(1, count, greet, 0)

    lanes = kernels.shape[2]
    depth = 2 * TAP**3
    def copy_to(plane, step):
        target = lax.rem(me + step, count)
        return pltpu.make_async_remote_copy(
            src_ref=sent.at[plane, target],
            dst_ref=held.at[plane, step],
            send_sem=send_sem.at[plane, step],
            recv_sem=recv_sem.at[plane, step],
            device_id={"slab": target},
            device_id_type=pl.DeviceIdType.MESH,
        )

    columns = kernels[...].reshape(depth, lanes)
    for plane in range(XD):
        images = jnp.dot(planes[plane, :, :depth], columns, preferred_element_type=jnp.float32)
        images = images + jnp.dot(planes[plane, :, depth:], columns, preferred_element_type=jnp.float32)
        for target in range(count):
            message = pack(images[target * PADROW : (target + 1) * PADROW], parts, width)
            sent[plane, target] = message.astype(jnp.bfloat16)
        if plane == 0:
            pl.semaphore_wait(barrier, count - 1)

        def send(step, carry):
            copy_to(plane, step).start()
            return carry

        lax.fori_loop(1, count, send, 0)

    column_count = count * lanes // COILS

    def settle(plane, source, block):
        moved = jnp.dot(place[...], block, preferred_element_type=jnp.float32).astype(jnp.bfloat16)
        for part in range(parts):
            start = source * lanes + part * width
            coil = start // column_count
            column = pl.multiple_of(lax.rem(start, column_count), width)
            taps[pl.ds(pl.multiple_of(coil * PADROW, PADROW), PADROW), pl.ds(column, width)] = moved[
                part * PADROW : (part + 1) * PADROW
            ]

    for plane in range(XD):
        settle(plane, me, sent[plane, me])

        def receive(step, carry):
            copy_to(plane, step).wait_recv()
            settle(plane, lax.rem(me - step + count, count), held[plane, step])
            return carry

        lax.fori_loop(1, count, receive, 0)
        gram_products(taps, swap, right.at[plane])

    for plane in range(XD):

        def drain(step, carry):
            copy_to(plane, step).wait_send()
            return carry

        lax.fori_loop(1, count, drain, 0)


def gram_products(taps, swap, right):
    group = LANES // COILS
    ordered = jnp.dot(swap[...], taps[...], preferred_element_type=jnp.float32).astype(jnp.bfloat16)
    products = lax.dot_general(
        taps[...], ordered, (((1,), (1,)), ((), ())), preferred_element_type=jnp.float32
    )
    lane = lax.broadcasted_iota(jnp.int32, (SUB, LANES), 1) // COILS
    level = lax.broadcasted_iota(jnp.int32, (SUB, LANES), 0)
    for block in range(COILS // group):
        picked = [[None] * ROW for _ in range(2)]
        for part in range(2):
            for row in range(ROW):
                place, start = row % group, row // group * LANES
                for member in range(group):
                    first = (block * group + member) * PADROW + part * SUB
                    piece = products[first : first + SUB, start : start + LANES]
                    turn = (member - place) % group * COILS
                    piece = pltpu.roll(piece, turn, axis=1) if turn else piece
                    known = picked[part][row]
                    picked[part][row] = piece if known is None else jnp.where(lane == member, piece, known)
        columns = slice(block * LANES, (block + 1) * LANES)
        for part in range(2):
            under, over = None, jnp.zeros((SUB, LANES), jnp.float32)
            for w in range(TAP):
                if part == 0:
                    value = picked[0][w] + picked[1][TAP + w]
                else:
                    value = picked[0][TAP + w] - picked[1][w]
                if w == 0:
                    under = value
                    continue
                value = pltpu.roll(value, w, axis=0)
                under = under + jnp.where(level >= w, value, 0.0)
                over = over + jnp.where(level < w, value, 0.0)
            right[part * PADROW : part * PADROW + SUB, columns] = under
            right[part * PADROW + SUB : (part + 1) * PADROW, columns] = over


def depth_kernel(right, table, out):
    value = right[0]
    high = value.astype(jnp.bfloat16)
    low = (value - high.astype(jnp.float32)).astype(jnp.bfloat16)
    stack = jnp.concatenate([high, high, low], axis=0)
    result = jnp.dot(table[...], stack, preferred_element_type=jnp.float32)
    out[0, 0, 0] = result[:NZ]
    out[1, 0, 0] = result[NZ:]


def local(kernels):
    count = lax.axis_size("slab")
    lanes = kernels.shape[4]
    column_count = count * lanes // COILS
    parts = 4 if lanes % (4 * LANES) == 0 else 1
    width = lanes // parts
    size = len(message_rows(parts))
    pairs = COILS * COILS
    vmem = pl.BlockSpec(memory_space=pltpu.VMEM)
    columns = jnp.transpose(kernels, (1, 2, 3, 0, 4)).reshape(TAP**3, 2, lanes)
    right = pl.pallas_call(
        functools.partial(exchange_kernel, count, parts, width),
        out_shape=jax.ShapeDtypeStruct((XD, 2 * PADROW, pairs), jnp.float32),
        in_specs=[vmem] * 4,
        out_specs=vmem,
        scratch_shapes=[
            pltpu.VMEM((XD, count, size, width), jnp.bfloat16),
            pltpu.VMEM((XD, count, size, width), jnp.bfloat16),
            pltpu.VMEM((COILS * PADROW, column_count), jnp.bfloat16),
            pltpu.SemaphoreType.DMA((XD, count)),
            pltpu.SemaphoreType.DMA((XD, count)),
        ],
        compiler_params=pltpu.CompilerParams(collective_id=0, has_side_effects=True),
        name="exchange",
    )(columns, jnp.asarray(plane_matrix(XD * count)), jnp.asarray(place_matrix(parts)), jnp.asarray(swap_matrix()))
    return pl.pallas_call(
        depth_kernel,
        grid=(XD, 2),
        out_shape=jax.ShapeDtypeStruct((2, XD, 1, NZ, pairs), jnp.float32),
        in_specs=[
            pl.BlockSpec((1, 2 * PADROW, pairs // 2), lambda plane, side: (plane, 0, side)),
            pl.BlockSpec((2 * NZ, 6 * PADROW), lambda plane, side: (0, 0)),
        ],
        out_specs=pl.BlockSpec((2, 1, 1, NZ, pairs // 2), lambda plane, side: (0, plane, 0, 0, side)),
        name="depth",
    )(right, jnp.asarray(depth_matrix()))


def solution(mesh):
    return jax.shard_map(
        local,
        mesh=mesh,
        in_specs=(P("scan", None, None, None, "slab"),),
        out_specs=P("scan", "slab", None, None, None),
        check_vma=False,
    )
```
